32 devices in a mesh: grp: 2 (over x), tile: 16 (over z, y, core).
Axes of the slice: x: 2, y: 2, z: 4, core: 2. Of those that a mesh axis runs over, the one named last changes fastest.
Arguments:
- voltages: bfloat16 [2, 32, 128, 1024], P(None, ('grp', 'tile')), parts along dimension 1, may hold values from -6 to 6
Outputs:
- visibilities: float32 [2, 2, 136, 128, 128], P(None, 'grp', None, 'tile'), parts along dimension 1
The draws below stay inside these ranges and needn't reach their ends.
There are 2 independent parts, one for each index of `grp`. The reference program is written for one: setup_inputs(seed, part) draws one part's arguments, and reference() takes and returns one part's arrays. A program takes and returns all parts, laid end to end along the dimension named above; each array names one. Nothing has to cross between parts.
All inputs are finite; a program needn't handle non-finite values.
Results may differ from the reference program's by a relative error of at most 0.0003.
Values may be sent and summed in bfloat16 or wider, within the bound.
No kernel may reach another device: no remote copies, remote signals or barrier semaphores. Data moves between devices by JAX's collectives and lax.ppermute only.
A program may use at most 64 MiB of HBM per device.

```python
import jax
import jax.numpy as jnp
import numpy as np
from jax import lax

NBLK = 16
TIME = 1024
BS = 128
CH = 1


def steps_of(key, dims, shards, least, top_value):
    def one(position, shards_of):
        heights = jax.random.uniform(jax.random.fold_in(jax.random.fold_in(key, 6), position), (shards_of,), jnp.float32, least / len(shards), top_value / len(shards))
        return jnp.repeat(jnp.exp(heights), dims[position] // shards_of).reshape((-1,) + (1,) * (len(dims) - position - 1))

    gain = one(*shards[0])
    for cut in shards[1:]:
        gain = gain * one(*cut)
    return gain


def centred(key, shape, spread, bound, shards=(), kind=jnp.bfloat16):
    loudness = steps_of(key, shape, shards, -0.22, 0.18) if shards else 1.0
    values = jax.random.normal(key, shape, jnp.float32) * spread * loudness
    return jnp.minimum(jnp.maximum(values, -bound), bound).astype(kind)


def setup_inputs(seed: int = 0, part: int = 0) -> dict:
    streams_of = jax.random.split(jax.random.key(seed), 2)
    part_splits = jax.random.split(jax.random.fold_in(streams_of[1], part), 2)
    return {
        "voltages": centred(part_splits[0], (2, NBLK * CH, BS, TIME), 1.0, 6.0, ((1, 16),)),
    }


def upper_pairs():
    row_list = []
    col_list = []
    for row_block in range(NBLK):
        for col_block in range(row_block, NBLK):
            row_list.append(row_block)
            col_list.append(col_block)
    return np.array(row_list, np.int32), np.array(col_list, np.int32)


def reference(voltages):
    row_index, col_index = upper_pairs()
    volts = voltages.astype(jnp.float32).reshape(2, NBLK, CH, BS, TIME)

    def channel_tiles(channel):
        data = lax.dynamic_index_in_dim(volts, channel, 2, keepdims=False)
        rows_side = data[:, row_index]
        cols_side = data[:, col_index]
        high = lax.Precision.HIGHEST
        real_part = jnp.einsum("kit,kjt->kij", rows_side[0], cols_side[0], precision=high) + jnp.einsum("kit,kjt->kij", rows_side[1], cols_side[1], precision=high)
        imag_part = jnp.einsum("kit,kjt->kij", rows_side[1], cols_side[0], precision=high) - jnp.einsum("kit,kjt->kij", rows_side[0], cols_side[1], precision=high)
        return jnp.stack([real_part, imag_part]) / TIME

    result = lax.map(channel_tiles, jnp.arange(CH, dtype=jnp.int32))
    return jnp.transpose(result, (1, 0, 2, 3, 4))
```

```python
import functools

import jax
import jax.numpy as jnp
from jax import lax
from jax.experimental import pallas as pl
from jax.experimental.pallas import tpu as pltpu
from jax.sharding import PartitionSpec as P

NBLK = 16
TIME = 1024


def unit_of(place, units):
    half = units // 2
    return 2 * place if place < half else 2 * (units - 1 - place) + 1


def ring_shift(block, lanes, split, shift):
    units = NBLK // lanes
    route = []
    for place in range(units):
        source = unit_of(place, units)
        target = unit_of((place + shift) % units, units)
        for lane in range(lanes):
            for channel in range(split):
                route.append(
                    (
                        (source * lanes + lane) * split + channel,
                        (target * lanes + lane) * split + channel,
                    )
                )
    return lax.ppermute(block, "tile", route)


def lane_swap(block, split):
    route = []
    for owner in range(NBLK):
        for channel in range(split):
            route.append((owner * split + channel, (owner ^ 1) * split + channel))
    return lax.ppermute(block, "tile", route)


def ring_gather(voltages, lanes, split):
    units = NBLK // lanes
    own = (voltages[0], voltages[1])
    held = [(0, own)]
    ahead, behind = own, own
    for step in range(1, units // 2):
        ahead = tuple(ring_shift(part, lanes, split, 1) for part in ahead)
        behind = tuple(ring_shift(part, lanes, split, -1) for part in behind)
        held.append((-step, ahead))
        held.append((step, behind))
    last = (ring_shift(ahead[0], lanes, split, 1), ring_shift(behind[1], lanes, split, -1))
    held.append((units // 2, last))
    slots = [(distance, 0, parts) for distance, parts in held]
    if lanes == 2:
        for distance, parts in held:
            slots.append((distance, 1, tuple(lane_swap(part, split) for part in parts)))
    return slots


def slot_blocks(slots, own_block, lanes):
    units = NBLK // lanes
    own_unit, own_lane = own_block // lanes, own_block % lanes
    own_place = jnp.where(own_unit % 2 == 0, own_unit // 2, units - 1 - own_unit // 2)
    distances = jnp.array([distance for distance, _, _ in slots], jnp.int32)
    flips = jnp.array([flip for _, flip, _ in slots], jnp.int32)
    places = (own_place + distances + units) % units
    unit = jnp.where(places < units // 2, 2 * places, 2 * (units - 1 - places) + 1)
    return unit * lanes + (own_lane + flips) % lanes


def tile_rows_kernel(count, index_ref, *refs):
    parts = refs[: 2 * count]
    out_ref, rows_ref = refs[2 * count :]
    own = index_ref[count]
    for slot in range(count):
        block = index_ref[slot]
        rows_ref[block] = parts[2 * slot][own]
        rows_ref[count + block] = parts[2 * slot + 1][own]
    chunks, height, time = rows_ref.shape
    rows = rows_ref[...].reshape(chunks * height, time)
    half = count * height
    dims = (((1,), (1,)), ((), ()))
    for slot in range(count):
        col = index_ref[slot]
        cols_re = parts[2 * slot][...].reshape(-1, time)
        cols_im = parts[2 * slot + 1][...].reshape(-1, time)
        with_re = lax.dot_general(rows, cols_re, dims, preferred_element_type=jnp.float32)
        with_im = lax.dot_general(rows, cols_im, dims, preferred_element_type=jnp.float32)
        real_part = (with_re[:half] + with_im[half:]) * (1.0 / TIME)
        imag_part = (with_re[half:] - with_im[:half]) * (1.0 / TIME)
        for row_block in reversed(range(count)):
            row = jnp.minimum(row_block, col)
            tile = row * count - row * (row - 1) // 2 + col - row
            span = slice(row_block * height, (row_block + 1) * height)
            out_ref[0, tile] = real_part[span]
            out_ref[1, tile] = imag_part[span]


def tile_rows(slots, blocks, own_block):
    count = len(slots)
    inputs, height = slots[0][2][0].shape[0], slots[0][2][0].shape[0] // NBLK
    time = slots[0][2][0].shape[1]
    parts = [part.reshape(NBLK, height, time) for _, _, pair in slots for part in pair]
    index = jnp.concatenate([blocks, own_block[None]]).astype(jnp.int32)
    vmem = pl.BlockSpec(memory_space=pltpu.VMEM)
    return pl.pallas_call(
        functools.partial(tile_rows_kernel, count),
        out_shape=jax.ShapeDtypeStruct((2, count * (count + 1) // 2, height, inputs), jnp.float32),
        in_specs=[pl.BlockSpec(memory_space=pltpu.SMEM)] + [vmem] * len(parts),
        out_specs=vmem,
        scratch_shapes=[pltpu.VMEM((2 * count, height, time), parts[0].dtype)],
        compiler_params=pltpu.CompilerParams(vmem_limit_bytes=20 * 2**20),
    )(index, *parts)


def on_device(voltages):
    split = lax.axis_size("tile") // NBLK
    lanes = 2 if split == 1 else 1
    own_block = lax.axis_index("tile") // split
    slots = ring_gather(voltages[:, 0], lanes, split)
    blocks = slot_blocks(slots, own_block, lanes)
    out = tile_rows(slots, blocks, own_block)[:, None]
    if split > 1:
        groups = [[owner * split + channel for channel in range(split)] for owner in range(NBLK)]
        out = lax.all_to_all(
            out, "tile", split_axis=3, concat_axis=1, axis_index_groups=groups, tiled=True
        )
    return out


def solution(mesh):
    placed = (P(None, ("grp", "tile"), None, None),)
    return jax.shard_map(
        on_device,
        mesh=mesh,
        in_specs=placed,
        out_specs=P(None, "grp", None, "tile", None),
        check_vma=False,
    )
```

```python
import functools

import jax
import jax.numpy as jnp
from jax import lax
from jax.experimental import pallas as pl
from jax.experimental.pallas import tpu as pltpu
from jax.sharding import PartitionSpec as P

NBLK = 16
TIME = 1024


def unit_of(place, units):
    half = units // 2
    return 2 * place if place < half else 2 * (units - 1 - place) + 1


def ring_shift(block, lanes, split, shift):
    units = NBLK // lanes
    route = []
    for place in range(units):
        source = unit_of(place, units)
        target = unit_of((place + shift) % units, units)
        for lane in range(lanes):
            for channel in range(split):
                route.append(
                    (
                        (source * lanes + lane) * split + channel,
                        (target * lanes + lane) * split + channel,
                    )
                )
    return lax.ppermute(block, "tile", route)


def lane_swap(block, split):
    route = []
    for owner in range(NBLK):
        for channel in range(split):
            route.append((owner * split + channel, (owner ^ 1) * split + channel))
    return lax.ppermute(block, "tile", route)


def ring_gather(voltages, lanes, split):
    units = NBLK // lanes

    def with_swaps(held):
        flipped = []
        if lanes == 2:
            flipped = [(d, 1, tuple(lane_swap(part, split) for part in parts)) for d, parts in held]
        return [(d, 0, parts) for d, parts in held] + flipped

    ahead = behind = (voltages[0], voltages[1])
    stages = []
    for step in range(1, units // 2):
        ahead = tuple(ring_shift(part, lanes, split, 1) for part in ahead)
        behind = tuple(ring_shift(part, lanes, split, -1) for part in behind)
        arrived = [(-step, ahead), (step, behind)]
        stages.append(with_swaps([(0, (voltages,))] + arrived if step == 1 else arrived))
    last = (ring_shift(ahead[0], lanes, split, 1), ring_shift(behind[1], lanes, split, -1))
    stages.append(with_swaps([(units // 2, last)]))
    return stages


def slot_blocks(slots, own_block, lanes):
    units = NBLK // lanes
    own_unit, own_lane = own_block // lanes, own_block % lanes
    own_place = jnp.where(own_unit % 2 == 0, own_unit // 2, units - 1 - own_unit // 2)
    distances = jnp.array([distance for distance, _, _ in slots] + [0], jnp.int32)
    flips = jnp.array([flip for _, flip, _ in slots] + [0], jnp.int32)
    places = (own_place + distances + units) % units
    unit = jnp.where(places < units // 2, 2 * places, 2 * (units - 1 - places) + 1)
    return unit * lanes + (own_lane + flips) % lanes


def stage_kernel(sizes, fresh, count, index_ref, *refs):
    known, old = len(sizes), len(sizes) - fresh
    arrays = list(refs[: sum(sizes)])
    out_ref, rows_ref, tiles_ref, sems = refs[-4:]
    parts = []
    for size in sizes:
        mine, arrays = arrays[:size], arrays[size:]
        parts.append([mine[0].at[0], mine[0].at[1]] if size == 1 else mine)
    height, time = rows_ref.shape[1:]
    own = index_ref[count]
    for slot, pair in enumerate(parts):
        for which in range(2):
            rows_ref[which * known + slot] = pair[which][own]
    rows = rows_ref[...].reshape(2 * known * height, time)
    if old:
        fresh_rows = jnp.concatenate(
            [rows_ref[old:known], rows_ref[known + old :]], axis=0
        ).reshape(2 * fresh * height, time)
    dims = (((1,), (1,)), ((), ()))

    def against(left, slot):
        half = left.shape[0] // 2
        with_re, with_im = (
            lax.dot_general(
                left, part[...].reshape(-1, time), dims, preferred_element_type=jnp.float32
            )
            for part in parts[slot]
        )
        real_part = (with_re[:half] + with_im[half:]) * (1.0 / time)
        imag_part = (with_re[half:] - with_im[:half]) * (1.0 / time)
        return real_part, imag_part

    as_cols = [against(rows, slot) for slot in range(old, known)]
    as_rows = [against(fresh_rows, slot) for slot in range(old)]
    copies = []
    for slot in range(old, known):
        mine = index_ref[slot]
        for other in range(slot + 1):
            theirs = index_ref[other]
            upper = theirs <= mine
            here = slice(other * height, (other + 1) * height)
            if other < old:
                flipped, there = as_rows[other], slice((slot - old) * height, (slot - old + 1) * height)
            else:
                flipped, there = as_cols[other - old], slice(slot * height, (slot + 1) * height)
            place = len(copies)
            for which in range(2):
                tiles_ref[place, which] = jnp.where(
                    upper, as_cols[slot - old][which][here], flipped[which][there]
                )
            low, high = jnp.minimum(mine, theirs), jnp.maximum(mine, theirs)
            tile = low * count - low * (low - 1) // 2 + high - low
            copy = pltpu.make_async_copy(tiles_ref.at[place], out_ref.at[:, tile], sems.at[place])
            copy.start()
            copies.append(copy)
    for copy in copies:
        copy.wait()


def stage_tiles(slots, fresh, index, tiles):
    known, old = len(slots), len(slots) - fresh
    count = index.shape[0] - 1
    inputs, time = slots[0][2][0].shape[-2:]
    height = inputs // NBLK
    parts = [
        part.reshape(part.shape[:-2] + (NBLK, height, time)) for _, _, held in slots for part in held
    ]
    pairs = fresh * (fresh + 1) // 2 + fresh * old
    vmem, anywhere = pl.BlockSpec(memory_space=pltpu.VMEM), pl.BlockSpec(memory_space=pl.ANY)
    shape = jax.ShapeDtypeStruct((2, count * (count + 1) // 2, height, inputs), jnp.float32)
    flops = 8 * height * inputs * time * (fresh * known + fresh * old)
    return pl.pallas_call(
        functools.partial(stage_kernel, [len(held) for _, _, held in slots], fresh, count),
        out_shape=shape,
        in_specs=[pl.BlockSpec(memory_space=pltpu.SMEM)]
        + [vmem] * len(parts)
        + ([] if tiles is None else [anywhere]),
        out_specs=anywhere,
        scratch_shapes=[
            pltpu.VMEM((2 * known, height, time), parts[0].dtype),
            pltpu.VMEM((pairs, 2, height, inputs), jnp.float32),
            pltpu.SemaphoreType.DMA((pairs,)),
        ],
        input_output_aliases={} if tiles is None else {1 + len(parts): 0},
        cost_estimate=pl.CostEstimate(flops=flops, bytes_accessed=2**20, transcendentals=0),
        compiler_params=pltpu.CompilerParams(vmem_limit_bytes=16 * 2**20),
    )(index, *parts, *([] if tiles is None else [tiles]))


def on_device(voltages):
    split = lax.axis_size("tile") // NBLK
    lanes = 2 if split == 1 else 1
    own_block = lax.axis_index("tile") // split
    stages = ring_gather(voltages[:, 0], lanes, split)
    index = slot_blocks([slot for stage in stages for slot in stage], own_block, lanes)
    slots, tiles = [], None
    for stage in stages:
        slots = slots + stage
        tiles = stage_tiles(slots, len(stage), index, tiles)
    out = tiles[:, None]
    if split > 1:
        groups = [[owner * split + channel for channel in range(split)] for owner in range(NBLK)]
        out = lax.all_to_all(
            out, "tile", split_axis=3, concat_axis=1, axis_index_groups=groups, tiled=True
        )
    return out


def solution(mesh):
    placed = (P(None, ("grp", "tile"), None, None),)
    return jax.shard_map(
        on_device,
        mesh=mesh,
        in_specs=placed,
        out_specs=P(None, "grp", None, "tile", None),
        check_vma=False,
    )
```

```python
import functools

import jax
import jax.numpy as jnp
from jax import lax
from jax.experimental import pallas as pl
from jax.experimental.pallas import tpu as pltpu
from jax.sharding import PartitionSpec as P

NBLK = 16
TIME = 1024


def unit_of(place, units):
    half = units // 2
    return 2 * place if place < half else 2 * (units - 1 - place) + 1


def ring_shift(block, lanes, split, shift):
    units = NBLK // lanes
    route = []
    for place in range(units):
        source = unit_of(place, units)
        target = unit_of((place + shift) % units, units)
        for lane in range(lanes):
            for channel in range(split):
                route.append(
                    (
                        (source * lanes + lane) * split + channel,
                        (target * lanes + lane) * split + channel,
                    )
                )
    return lax.ppermute(block, "tile", route)


def lane_swap(block, split):
    route = []
    for owner in range(NBLK):
        for channel in range(split):
            route.append((owner * split + channel, (owner ^ 1) * split + channel))
    return lax.ppermute(block, "tile", route)


def ring_gather(voltages, lanes, split):
    units = NBLK // lanes

    def with_swaps(held):
        flipped = []
        if lanes == 2:
            flipped = [(d, 1, tuple(lane_swap(part, split) for part in parts)) for d, parts in held]
        return [(d, 0, parts) for d, parts in held] + flipped

    ahead = behind = (voltages[0], voltages[1])
    stages = []
    for step in range(1, units // 2):
        ahead = tuple(ring_shift(part, lanes, split, 1) for part in ahead)
        behind = tuple(ring_shift(part, lanes, split, -1) for part in behind)
        arrived = [(-step, ahead), (step, behind)]
        stages.append(with_swaps([(0, (voltages,))] + arrived if step == 1 else arrived))
    last = (ring_shift(ahead[0], lanes, split, 1), ring_shift(behind[1], lanes, split, -1))
    stages.append(with_swaps([(units // 2, last)]))
    return stages


def slot_blocks(slots, own_block, lanes):
    units = NBLK // lanes
    own_unit, own_lane = own_block // lanes, own_block % lanes
    own_place = jnp.where(own_unit % 2 == 0, own_unit // 2, units - 1 - own_unit // 2)
    distances = jnp.array([distance for distance, _, _ in slots] + [0], jnp.int32)
    flips = jnp.array([flip for _, flip, _ in slots] + [0], jnp.int32)
    places = (own_place + distances + units) % units
    unit = jnp.where(places < units // 2, 2 * places, 2 * (units - 1 - places) + 1)
    return unit * lanes + (own_lane + flips) % lanes


def tiles_kernel(sizes, index_ref, *refs):
    count = len(sizes)
    arrays = list(refs[: sum(sizes)])
    out_ref, rows_ref = refs[-2:]
    parts = []
    for size in sizes:
        mine, arrays = arrays[:size], arrays[size:]
        parts.append([mine[0].at[0], mine[0].at[1]] if size == 1 else mine)
    height, time = rows_ref.shape[1:]
    own = index_ref[count]
    for slot, pair in enumerate(parts):
        block = index_ref[slot]
        rows_ref[block] = pair[0][own]
        rows_ref[count + block] = pair[1][own]
    half = count * height
    rows = rows_ref[...].reshape(2 * half, time)
    for slot, pair in enumerate(parts):
        col = index_ref[slot]
        cols = jnp.concatenate([part[...].reshape(-1, time) for part in pair], axis=0)
        width = cols.shape[0] // 2
        both = lax.dot_general(
            rows, cols, (((1,), (1,)), ((), ())), preferred_element_type=jnp.float32
        )
        real_part = (both[:half, :width] + both[half:, width:]) * (1.0 / time)
        imag_part = (both[half:, :width] - both[:half, width:]) * (1.0 / time)
        for row_block in reversed(range(count)):
            row = jnp.minimum(row_block, col)
            tile = row * count - row * (row - 1) // 2 + col - row
            span = slice(row_block * height, (row_block + 1) * height)
            out_ref[0, tile] = real_part[span]
            out_ref[1, tile] = imag_part[span]


def all_tiles(slots, index):
    count = len(slots)
    inputs, time = slots[0][2][0].shape[-2:]
    height = inputs // NBLK
    parts = [
        part.reshape(part.shape[:-2] + (NBLK, height, time)) for _, _, held in slots for part in held
    ]
    parts = [pltpu.with_memory_space_constraint(part, pltpu.VMEM) for part in parts]
    vmem = pl.BlockSpec(memory_space=pltpu.VMEM)
    return pl.pallas_call(
        functools.partial(tiles_kernel, [len(held) for _, _, held in slots]),
        out_shape=jax.ShapeDtypeStruct((2, count * (count + 1) // 2, height, inputs), jnp.float32),
        in_specs=[pl.BlockSpec(memory_space=pltpu.SMEM)] + [vmem] * len(parts),
        out_specs=vmem,
        scratch_shapes=[pltpu.VMEM((2 * count, height, time), parts[0].dtype)],
        compiler_params=pltpu.CompilerParams(vmem_limit_bytes=16 * 2**20),
    )(index, *parts)


def on_device(voltages):
    split = lax.axis_size("tile") // NBLK
    lanes = 2 if split == 1 else 1
    own_block = lax.axis_index("tile") // split
    stages = ring_gather(voltages[:, 0], lanes, split)
    index = slot_blocks([slot for stage in stages for slot in stage], own_block, lanes)
    out = all_tiles([slot for stage in stages for slot in stage], index)[:, None]
    if split > 1:
        groups = [[owner * split + channel for channel in range(split)] for owner in range(NBLK)]
        out = lax.all_to_all(
            out, "tile", split_axis=3, concat_axis=1, axis_index_groups=groups, tiled=True
        )
    return out


def solution(mesh):
    placed = (P(None, ("grp", "tile"), None, None),)
    return jax.shard_map(
        on_device,
        mesh=mesh,
        in_specs=placed,
        out_specs=P(None, "grp", None, "tile", None),
        check_vma=False,
    )
```

```python
import functools

import jax
import jax.numpy as jnp
from jax import lax
from jax.experimental import pallas as pl
from jax.experimental.pallas import tpu as pltpu
from jax.sharding import PartitionSpec as P

NBLK = 16
TIME = 1024


def unit_of(place, units):
    half = units // 2
    return 2 * place if place < half else 2 * (units - 1 - place) + 1


def ring_shift(block, lanes, split, shift):
    units = NBLK // lanes
    route = []
    for place in range(units):
        source = unit_of(place, units)
        target = unit_of((place + shift) % units, units)
        for lane in range(lanes):
            for channel in range(split):
                route.append(
                    (
                        (source * lanes + lane) * split + channel,
                        (target * lanes + lane) * split + channel,
                    )
                )
    return lax.ppermute(block, "tile", route)


def lane_swap(block, split):
    route = []
    for owner in range(NBLK):
        for channel in range(split):
            route.append((owner * split + channel, (owner ^ 1) * split + channel))
    return lax.ppermute(block, "tile", route)


def ring_gather(voltages, lanes, split):
    units = NBLK // lanes

    def with_swaps(held):
        flipped = []
        if lanes == 2:
            flipped = [(d, 1, tuple(lane_swap(part, split) for part in parts)) for d, parts in held]
        return [(d, 0, parts) for d, parts in held] + flipped

    ahead = behind = (voltages[0], voltages[1])
    stages = []
    for step in range(1, units // 2):
        ahead = tuple(ring_shift(part, lanes, split, 1) for part in ahead)
        behind = tuple(ring_shift(part, lanes, split, -1) for part in behind)
        arrived = [(-step, ahead), (step, behind)]
        stages.append(with_swaps([(0, (voltages,))] + arrived if step == 1 else arrived))
    last = (ring_shift(ahead[0], lanes, split, 1), ring_shift(behind[1], lanes, split, -1))
    stages.append(with_swaps([(units // 2, last)]))
    return stages


def slot_blocks(slots, own_block, lanes):
    units = NBLK // lanes
    own_unit, own_lane = own_block // lanes, own_block % lanes
    own_place = jnp.where(own_unit % 2 == 0, own_unit // 2, units - 1 - own_unit // 2)
    distances = jnp.array([distance for distance, _, _ in slots], jnp.int32)
    flips = jnp.array([flip for _, flip, _ in slots], jnp.int32)
    places = (own_place + distances + units) % units
    unit = jnp.where(places < units // 2, 2 * places, 2 * (units - 1 - places) + 1)
    blocks = unit * lanes + (own_lane + flips) % lanes
    return jnp.concatenate([blocks, own_block[None]]).astype(jnp.int32)


def tiles_kernel(sizes, index_ref, *refs):
    count = len(sizes)
    arrays = list(refs[: sum(sizes)])
    out_ref, rows_ref = refs[-2:]
    parts = []
    for size in sizes:
        mine, arrays = arrays[:size], arrays[size:]
        parts.append([mine[0].at[0], mine[0].at[1]] if size == 1 else mine)
    height, time = rows_ref.shape[1:]
    own = index_ref[count]
    for slot, pair in enumerate(parts):
        block = index_ref[slot]
        rows_ref[block] = pair[0][own]
        rows_ref[count + block] = pair[1][own]
    half = count * height
    rows = rows_ref[...].reshape(2 * half, time)
    for slot, pair in enumerate(parts):
        col = index_ref[slot]
        cols = jnp.concatenate([part[...].reshape(-1, time) for part in pair], axis=0)
        width = cols.shape[0] // 2
        both = lax.dot_general(
            rows, cols, (((1,), (1,)), ((), ())), preferred_element_type=jnp.float32
        )
        real_part = (both[:half, :width] + both[half:, width:]) * (1.0 / time)
        imag_part = (both[half:, :width] - both[:half, width:]) * (1.0 / time)
        for row_block in reversed(range(count)):
            row = jnp.minimum(row_block, col)
            tile = row * count - row * (row - 1) // 2 + col - row
            span = slice(row_block * height, (row_block + 1) * height)
            out_ref[0, tile] = real_part[span]
            out_ref[1, tile] = imag_part[span]


def all_tiles(slots, index):
    count = len(slots)
    inputs, time = slots[0][2][0].shape[-2:]
    height = inputs // NBLK
    parts = [
        part.reshape(part.shape[:-2] + (NBLK, height, time)) for _, _, held in slots for part in held
    ]
    parts = [pltpu.with_memory_space_constraint(part, pltpu.VMEM) for part in parts]
    vmem = pl.BlockSpec(memory_space=pltpu.VMEM)
    return pl.pallas_call(
        functools.partial(tiles_kernel, [len(held) for _, _, held in slots]),
        out_shape=jax.ShapeDtypeStruct((2, count * (count + 1) // 2, height, inputs), jnp.float32),
        in_specs=[pl.BlockSpec(memory_space=pltpu.SMEM)] + [vmem] * len(parts),
        out_specs=vmem,
        scratch_shapes=[pltpu.VMEM((2 * count, height, time), parts[0].dtype)],
        compiler_params=pltpu.CompilerParams(vmem_limit_bytes=16 * 2**20),
    )(index, *parts)


def on_device(voltages):
    split = lax.axis_size("tile") // NBLK
    lanes = 2 if split == 1 else 1
    own_block = lax.axis_index("tile") // split
    stages = ring_gather(voltages[:, 0], lanes, split)
    index = slot_blocks([slot for stage in stages for slot in stage], own_block, lanes)
    out = all_tiles([slot for stage in stages for slot in stage], index)[:, None]
    if split > 1:
        groups = [[owner * split + channel for channel in range(split)] for owner in range(NBLK)]
        out = lax.all_to_all(
            out, "tile", split_axis=3, concat_axis=1, axis_index_groups=groups, tiled=True
        )
    return out


def solution(mesh):
    placed = (P(None, ("grp", "tile"), None, None),)
    return jax.shard_map(
        on_device,
        mesh=mesh,
        in_specs=placed,
        out_specs=P(None, "grp", None, "tile", None),
        check_vma=False,
    )
```

```python
import functools

import jax
import jax.numpy as jnp
from jax import lax
from jax.experimental import pallas as pl
from jax.experimental.pallas import tpu as pltpu
from jax.sharding import PartitionSpec as P

NBLK = 16
TIME = 1024


def unit_of(place, units):
    half = units // 2
    return 2 * place if place < half else 2 * (units - 1 - place) + 1


def ring_shift(block, lanes, split, shift):
    units = NBLK // lanes
    route = []
    for place in range(units):
        source = unit_of(place, units)
        target = unit_of((place + shift) % units, units)
        for lane in range(lanes):
            for channel in range(split):
                route.append(
                    (
                        (source * lanes + lane) * split + channel,
                        (target * lanes + lane) * split + channel,
                    )
                )
    return lax.ppermute(block, "tile", route)


def lane_swap(block, split):
    route = []
    for owner in range(NBLK):
        for channel in range(split):
            route.append((owner * split + channel, (owner ^ 1) * split + channel))
    return lax.ppermute(block, "tile", route)


def ring_gather(voltages, lanes, split):
    units = NBLK // lanes

    def with_swaps(held):
        flipped = []
        if lanes == 2:
            flipped = [(d, 1, tuple(lane_swap(part, split) for part in parts)) for d, parts in held]
        return [(d, 0, parts) for d, parts in held] + flipped

    ahead = behind = (voltages[0], voltages[1])
    stages = []
    for step in range(1, units // 2):
        ahead = tuple(ring_shift(part, lanes, split, 1) for part in ahead)
        behind = tuple(ring_shift(part, lanes, split, -1) for part in behind)
        arrived = [(-step, ahead), (step, behind)]
        stages.append(with_swaps([(0, (voltages,))] + arrived if step == 1 else arrived))
    last = (ring_shift(ahead[0], lanes, split, 1), ring_shift(behind[1], lanes, split, -1))
    stages.append(with_swaps([(units // 2, last)]))
    return stages


def slot_blocks(slots, own_block, lanes):
    units = NBLK // lanes
    own_unit, own_lane = lax.div(own_block, lanes), lax.rem(own_block, lanes)
    column, side = lax.div(own_unit, 2), lax.rem(own_unit, 2)
    own_place = jnp.where(side == 0, column, units - 1 - column)
    blocks = []
    for distance, flip in slots:
        place = lax.rem(own_place + distance + units, units)
        unit = jnp.where(place < units // 2, 2 * place, 2 * (units - 1 - place) + 1)
        lane = 1 - own_lane if flip else own_lane
        blocks.append(unit * lanes + lane)
    return blocks


def tiles_kernel(sizes, slots, lanes, split, *refs):
    count = len(sizes)
    arrays = list(refs[: sum(sizes)])
    out_ref, rows_ref = refs[-2:]
    parts = []
    for size in sizes:
        mine, arrays = arrays[:size], arrays[size:]
        parts.append([mine[0].at[0], mine[0].at[1]] if size == 1 else mine)
    height, time = rows_ref.shape[1:]
    own = lax.div(lax.axis_index("tile"), split)
    blocks = slot_blocks(slots, own, lanes)
    for slot, pair in enumerate(parts):
        block = blocks[slot]
        rows_ref[block] = pair[0][own]
        rows_ref[count + block] = pair[1][own]
    half = count * height
    rows = rows_ref[...].reshape(2 * half, time)
    for slot, pair in enumerate(parts):
        col = blocks[slot]
        cols = jnp.concatenate([part[...].reshape(-1, time) for part in pair], axis=0)
        width = cols.shape[0] // 2
        both = lax.dot_general(
            rows, cols, (((1,), (1,)), ((), ())), preferred_element_type=jnp.float32
        )
        real_part = (both[:half, :width] + both[half:, width:]) * (1.0 / time)
        imag_part = (both[half:, :width] - both[:half, width:]) * (1.0 / time)
        for row_block in reversed(range(count)):
            row = jnp.minimum(row_block, col)
            tile = row * count - row * (row - 1) // 2 + col - row
            span = slice(row_block * height, (row_block + 1) * height)
            out_ref[0, tile] = real_part[span]
            out_ref[1, tile] = imag_part[span]


def all_tiles(slots, lanes, split):
    count = len(slots)
    inputs, time = slots[0][2][0].shape[-2:]
    height = inputs // NBLK
    parts = [
        part.reshape(part.shape[:-2] + (NBLK, height, time)) for _, _, held in slots for part in held
    ]
    vmem = pl.BlockSpec(memory_space=pltpu.VMEM)
    return pl.pallas_call(
        functools.partial(
            tiles_kernel,
            [len(held) for _, _, held in slots],
            [slot[:2] for slot in slots],
            lanes,
            split,
        ),
        out_shape=jax.ShapeDtypeStruct((2, count * (count + 1) // 2, height, inputs), jnp.float32),
        in_specs=[vmem] * len(parts),
        out_specs=vmem,
        scratch_shapes=[pltpu.VMEM((2 * count, height, time), parts[0].dtype)],
        compiler_params=pltpu.CompilerParams(vmem_limit_bytes=16 * 2**20),
    )(*parts)


def on_device(voltages):
    split = lax.axis_size("tile") // NBLK
    lanes = 2 if split == 1 else 1
    stages = ring_gather(voltages[:, 0], lanes, split)
    out = all_tiles([slot for stage in stages for slot in stage], lanes, split)[:, None]
    if split > 1:
        groups = [[owner * split + channel for channel in range(split)] for owner in range(NBLK)]
        out = lax.all_to_all(
            out, "tile", split_axis=3, concat_axis=1, axis_index_groups=groups, tiled=True
        )
    return out


def solution(mesh):
    placed = (P(None, ("grp", "tile"), None, None),)
    return jax.shard_map(
        on_device,
        mesh=mesh,
        in_specs=placed,
        out_specs=P(None, "grp", None, "tile", None),
        check_vma=False,
    )
```

```python
import functools

import jax
import jax.numpy as jnp
from jax import lax
from jax.experimental import pallas as pl
from jax.experimental.pallas import tpu as pltpu
from jax.sharding import PartitionSpec as P

NBLK = 16


def unit_of(place, units):
    half = units // 2
    return 2 * place if place < half else 2 * (units - 1 - place) + 1


def ring_shift(block, lanes, split, shift):
    units = NBLK // lanes
    route = []
    for place in range(units):
        source = unit_of(place, units)
        target = unit_of((place + shift) % units, units)
        for lane in range(lanes):
            for channel in range(split):
                route.append(
                    (
                        (source * lanes + lane) * split + channel,
                        (target * lanes + lane) * split + channel,
                    )
                )
    return lax.ppermute(block, "tile", route)


def lane_swap(block, split):
    route = []
    for owner in range(NBLK):
        for channel in range(split):
            route.append((owner * split + channel, (owner ^ 1) * split + channel))
    return lax.ppermute(block, "tile", route)


def ring_gather(voltages, lanes, split):
    units = NBLK // lanes

    def shift(block, way):
        return ring_shift(block, lanes, split, way)

    def with_swaps(held):
        flipped = []
        if lanes == 2:
            flipped = [(d, 1, tuple(lane_swap(part, split) for part in parts)) for d, parts in held]
        return [(d, 0, parts) for d, parts in held] + flipped

    ahead = behind = (voltages[0], voltages[1])
    stages = []
    for step in range(1, units // 2):
        ahead = tuple(shift(part, 1) for part in ahead)
        behind = tuple(shift(part, -1) for part in behind)
        arrived = [(-step, ahead), (step, behind)]
        stages.append(with_swaps([(0, (voltages,))] + arrived if step == 1 else arrived))
    last = (shift(ahead[0], 1), shift(behind[1], -1))
    stages.append(with_swaps([(units // 2, last)]))
    return stages


def slot_blocks(slots, own_block, lanes):
    units = NBLK // lanes
    own_unit, own_lane = lax.div(own_block, lanes), lax.rem(own_block, lanes)
    column, side = lax.div(own_unit, 2), lax.rem(own_unit, 2)
    own_place = jnp.where(side == 0, column, units - 1 - column)
    blocks = []
    for distance, flip in slots:
        place = lax.rem(own_place + distance + units, units)
        unit = jnp.where(place < units // 2, 2 * place, 2 * (units - 1 - place) + 1)
        lane = 1 - own_lane if flip else own_lane
        blocks.append(unit * lanes + lane)
    return blocks


def tiles_kernel(sizes, slots, lanes, split, *refs):
    count = len(sizes)
    arrays = list(refs[: sum(sizes)])
    out_ref, rows_ref = refs[-2:]
    parts = []
    for size in sizes:
        mine, arrays = arrays[:size], arrays[size:]
        parts.append([mine[0].at[0], mine[0].at[1]] if size == 1 else mine)
    height, time = rows_ref.shape[1:]
    own = lax.div(lax.axis_index("tile"), split)
    blocks = slot_blocks(slots, own, lanes)
    for slot, pair in enumerate(parts):
        block = blocks[slot]
        rows_ref[block] = pair[0][own]
        rows_ref[count + block] = pair[1][own]
    half = count * height
    rows = rows_ref[...].reshape(2 * half, time)
    for slot, pair in enumerate(parts):
        col = blocks[slot]
        cols = jnp.concatenate([part[...].reshape(-1, time) for part in pair], axis=0)
        width = cols.shape[0] // 2
        both = lax.dot_general(
            rows, cols, (((1,), (1,)), ((), ())), preferred_element_type=jnp.float32
        )
        real_part = (both[:half, :width] + both[half:, width:]) * (1.0 / time)
        imag_part = (both[half:, :width] - both[:half, width:]) * (1.0 / time)
        for row_block in reversed(range(count)):
            row = jnp.minimum(row_block, col)
            tile = row * count - row * (row - 1) // 2 + col - row
            span = slice(row_block * height, (row_block + 1) * height)
            out_ref[0, tile] = real_part[span]
            out_ref[1, tile] = imag_part[span]


def all_tiles(slots, lanes, split):
    count = len(slots)
    inputs, time = slots[0][2][0].shape[-2:]
    height = inputs // NBLK
    parts = [
        part.reshape(part.shape[:-2] + (NBLK, height, time)) for _, _, held in slots for part in held
    ]
    vmem = pl.BlockSpec(memory_space=pltpu.VMEM)
    return pl.pallas_call(
        functools.partial(
            tiles_kernel,
            [len(held) for _, _, held in slots],
            [slot[:2] for slot in slots],
            lanes,
            split,
        ),
        out_shape=jax.ShapeDtypeStruct((2, count * (count + 1) // 2, height, inputs), jnp.float32),
        in_specs=[vmem] * len(parts),
        out_specs=vmem,
        scratch_shapes=[pltpu.VMEM((2 * count, height, time), parts[0].dtype)],
        compiler_params=pltpu.CompilerParams(vmem_limit_bytes=16 * 2**20),
    )(*parts)


def on_device(voltages):
    split = lax.axis_size("tile") // NBLK
    lanes = 2 if split == 1 else 1
    stages = ring_gather(voltages[:, 0], lanes, split)
    out = all_tiles([slot for stage in stages for slot in stage], lanes, split)[:, None]
    if split > 1:
        groups = [[owner * split + channel for channel in range(split)] for owner in range(NBLK)]
        out = lax.all_to_all(
            out, "tile", split_axis=3, concat_axis=1, axis_index_groups=groups, tiled=True
        )
    return out


def solution(mesh):
    placed = (P(None, ("grp", "tile"), None, None),)
    return jax.shard_map(
        on_device,
        mesh=mesh,
        in_specs=placed,
        out_specs=P(None, "grp", None, "tile", None),
        check_vma=False,
    )
```
